32 devices in a mesh: img: 8 (over y, x, core), atom: 4 (over z).
Axes of the slice: x: 2, y: 2, z: 4, core: 2. Of those that a mesh axis runs over, the one named last changes fastest.
Arguments:
- positions: float32 [3, 256, 4096], P(None, 'img', 'atom'), may hold values from -6 to 6
- strength: float32 [4096], replicated, may hold values from 0.5 to 2
- tile_pairs: int32 [32, 8], replicated, may hold values from 0 to 31
- source_segment: int32 [256], P('img'), may hold values from 1 to 255, as said below
Outputs:
- string: float32 [3, 256, 4096], P(None, 'img', 'atom')
The draws below stay inside these ranges and needn't reach their ends.
Inputs may be any that keep to these rules, and one draw needn't show every extreme that they name: source_segment[j] is j or j + 1, never 0 and never above 255.
All inputs are finite; a program needn't handle non-finite values.
Results may differ from the reference program's by a relative error of at most 0.0003.
Values sent between devices are 32-bit elements; how exact they have to be, the bound alone decides.
A program may use at most 64 MiB of HBM per device.

```python
import math
import jax
import jax.numpy as jnp
from jax import lax

NA = 4096
TB = 128
K = 8
NBLK = 32
IMAGES = 256


def draw_source_segment(key, part):
    bump = jax.random.randint(key, (IMAGES,), 0, 2).astype(jnp.int32)
    return jnp.clip(jnp.arange(IMAGES, dtype=jnp.int32) + bump, 1, IMAGES - 1).astype(jnp.int32)


def touch_ends(result, own_key, low, largest):
    shape = result.shape
    spot = [jax.random.randint(jax.random.fold_in(own_key, axis), (), 0, shape[axis]) for axis in range(len(shape))]
    result = result.at[tuple(spot)].set(low)
    longest = shape.index(max(shape))
    spot[longest] = (spot[longest] + 1) % shape[longest]
    return result.at[tuple(spot)].set(largest)


def block_scale(key, dims, shards, low, high):
    def one(axis_at, parts):
        steps = jax.random.uniform(jax.random.fold_in(jax.random.fold_in(key, 6), axis_at), (parts,), jnp.float32, low / len(shards), high / len(shards))
        return jnp.repeat(jnp.exp(steps), dims[axis_at] // parts).reshape((-1,) + (1,) * (len(dims) - axis_at - 1))

    level = one(*shards[0])
    for cut in shards[1:]:
        level = level * one(*cut)
    return level


def bell_draw(key, dims, deviation, most, shards=(), kind=jnp.bfloat16):
    loudness = block_scale(key, dims, shards, -0.22, 0.18) if shards else 1.0
    array = jax.random.normal(key, dims, jnp.float32) * deviation * loudness
    return jnp.minimum(jnp.maximum(array, -most), most).astype(kind)


def setup_inputs(seed: int = 0) -> dict:
    arg_keys = jax.random.split(jax.random.key(seed), 5)
    positions = bell_draw(arg_keys[0], (3, IMAGES, NA), 1.0, 6.0, ((1, 8), (2, 4)), jnp.float32)
    strength = jnp.clip(jnp.exp(jax.random.uniform(arg_keys[1], (NA,), jnp.float32, math.log(0.5), math.log(2.0))), 0.5, 2.0)
    tile_pairs = touch_ends(jax.random.randint(arg_keys[2], (NBLK, K), 0, NBLK), jax.random.fold_in(arg_keys[2], 1), 0, NBLK - 1).astype(jnp.int32)
    source_segment = draw_source_segment(jax.random.fold_in(arg_keys[4], 71), 0)
    return dict(positions=positions, strength=strength, tile_pairs=tile_pairs, source_segment=source_segment)


STEP_SIZE = 0.02

def pair_force(block_pos, block_strength, whole_pos, strength, partners):
    force_sum = jnp.zeros(block_pos.shape, jnp.float32)
    for neighbor_slot in range(partners.shape[0]):
        first_atom = (partners[neighbor_slot] * TB).astype(jnp.int32)
        partner_pos = lax.dynamic_slice_in_dim(whole_pos, first_atom, TB, 2)
        partner_strength = lax.dynamic_slice_in_dim(strength, first_atom, TB, 0)
        differ = block_pos[:, :, :, None] - partner_pos[:, :, None, :]
        radius = lax.optimization_barrier(jnp.sum(differ * differ, axis=0))
        coupling = block_strength[None, :, None] * partner_strength[None, None, :] * jnp.exp(-0.5 * radius)
        force_sum = force_sum + lax.optimization_barrier(jnp.sum(differ * coupling[None], axis=3))
    return force_sum

def reference(positions, strength, tile_pairs, source_segment):
    blocks = positions.reshape(3, IMAGES, NBLK, TB).transpose(2, 0, 1, 3)

    def one_block(inputs):
        block_pos, index = inputs
        partners = tile_pairs[index]
        block_strength = lax.dynamic_slice_in_dim(strength, (index * TB).astype(jnp.int32), TB, 0)
        return pair_force(block_pos, block_strength, positions, strength, partners)
    forces = lax.map(one_block, (blocks, jnp.arange(NBLK, dtype=jnp.int32)))
    forces = forces.transpose(1, 2, 0, 3).reshape(3, IMAGES, NA)
    moved = positions + STEP_SIZE * forces
    deltas = moved[:, 1:] - moved[:, :-1]
    squares = lax.optimization_barrier(jnp.sum(deltas * deltas, axis=(0, 2)))
    lengths = jnp.concatenate([jnp.zeros((1,), jnp.float32), jnp.sqrt(1.0 + squares)])
    arc = jnp.cumsum(lengths)
    total_arc = arc[-1]
    target = jnp.arange(IMAGES).astype(jnp.float32) * (total_arc / (IMAGES - 1))
    lower = (source_segment - 1).astype(jnp.int32)
    weight = (target - arc[lower]) / lengths[source_segment]
    string = (1.0 - weight)[None, :, None] * moved[:, lower] + weight[None, :, None] * moved[:, source_segment]
    return string
```

```python
import functools
import math

import jax
import jax.numpy as jnp
from jax import lax
from jax.experimental import pallas as pl
from jax.experimental.pallas import tpu as pltpu
from jax.sharding import PartitionSpec as P

TB = 128
STEP_SIZE = 0.02
LOG2E = math.log2(math.e)
F32 = jnp.float32
BF16 = jnp.bfloat16


def split3(v):
    h = v.astype(BF16).astype(F32)
    r = v - h
    m = r.astype(BF16).astype(F32)
    return h, m, r - m


def features(x0, x1, x2, logs):
    shape = (8, x0.shape[1])
    row = lax.broadcasted_iota(jnp.int32, shape, 0)
    comp = row & 3
    low = row < 4
    half = (-0.5 * LOG2E) * (x0 * x0 + x1 * x1 + x2 * x2)
    x0, x1, x2 = (jnp.broadcast_to(v, shape) for v in (x0, x1, x2))
    norm_j = jnp.broadcast_to(half + logs, shape)
    norm_i = jnp.broadcast_to(half, shape)
    xs = jnp.where(comp == 0, x0, jnp.where(comp == 1, x1, x2))
    h, m, l = split3(jnp.where(comp == 3, norm_j, xs))
    ones = jnp.where(row < 3, 1.0, 0.0).astype(F32)
    key = jnp.concatenate([h, jnp.where(low, h, m), jnp.where(low, m, l), ones], axis=0)
    bh, bm, bl = split3(jnp.where(comp == 3, 1.0, LOG2E * xs))
    ph, pm, plo = split3(norm_i)
    tail = jnp.where(row == 0, ph, jnp.where(row == 1, pm, jnp.where(row == 2, plo, 0.0)))
    query = jnp.concatenate(
        [jnp.where(low, bh, bm), jnp.where(low, bl, bh), jnp.where(low, bm, bh), tail], axis=0
    )
    v0 = jnp.where(comp == 3, jnp.where(low, 1.0, 0.0), jnp.where(low, h, m))
    v1 = jnp.where(row < 3, l, 0.0)
    value = jnp.concatenate([v0, v1], axis=0)
    return query, key, value


def force_kernel(x_ref, s_ref, pairs_ref, out_ref, query_ref, key_ref, value_ref):
    images = x_ref.shape[1]
    tiles = x_ref.shape[2] // TB
    neighbors = pairs_ref.shape[1]

    for pair in range(images // 2):

        @pl.loop(0, tiles)
        def _(t, pair=pair):
            lanes = pl.ds(pl.multiple_of(t * TB, TB), TB)
            logs = jnp.log2(s_ref[:, lanes])
            (qa, ka, va), (qb, kb, vb) = (
                features(*(x_ref[c, pl.ds(image, 1), lanes] for c in range(3)), logs)
                for image in (2 * pair, 2 * pair + 1)
            )
            zero = jnp.zeros_like(qa)
            query_ref[pair, t] = jnp.concatenate(
                [jnp.concatenate([qa, zero], axis=1), jnp.concatenate([zero, qb], axis=1)], axis=0
            ).astype(BF16)
            keys = jnp.concatenate([ka, kb, jnp.zeros_like(ka), jnp.zeros_like(kb)], axis=0)
            key_ref[pair, t] = keys.T.astype(BF16)
            values = jnp.concatenate([va, vb], axis=0).astype(BF16)
            value_ref[pair, t] = jnp.concatenate([values, values], axis=1)

    for pair in range(images // 2):

        @pl.loop(0, tiles)
        def _(b, pair=pair):
            query = query_ref[pair, b]
            total = jnp.zeros((32, 2 * TB), F32)
            for slot in range(neighbors):
                t = pairs_ref[b, slot]
                power = jnp.dot(key_ref[pair, t][:, :64], query, preferred_element_type=F32)
                weight = jnp.exp2(power)
                hi = weight.astype(BF16)
                lo = (weight - hi.astype(F32)).astype(BF16)
                total = total + jnp.dot(
                    value_ref[pair, t],
                    jnp.concatenate([hi, lo], axis=0),
                    preferred_element_type=F32,
                )
            lanes = pl.ds(pl.multiple_of(b * TB, TB), TB)
            step = STEP_SIZE * s_ref[:, lanes]
            for side in range(2):
                block = total[16 * side : 16 * side + 16, side * TB : (side + 1) * TB]
                weight_sum = block[3:4]
                for c in range(3):
                    moment = block[c : c + 1] + block[4 + c : 5 + c] + block[8 + c : 9 + c]
                    x = x_ref[c, pl.ds(2 * pair + side, 1), lanes]
                    out_ref[c, pl.ds(2 * pair + side, 1), lanes] = x + step * (
                        x * weight_sum - moment
                    )


def moved_images(x, strength, tile_pairs):
    _, images, atoms = x.shape
    tiles = atoms // TB
    pairs = images // 2
    vmem = pl.BlockSpec(memory_space=pltpu.VMEM)
    return pl.pallas_call(
        force_kernel,
        out_shape=jax.ShapeDtypeStruct(x.shape, F32),
        in_specs=[vmem, vmem, pl.BlockSpec(memory_space=pltpu.SMEM)],
        out_specs=vmem,
        scratch_shapes=[
            pltpu.VMEM((pairs, tiles, 64, 2 * TB), BF16),
            pltpu.VMEM((pairs, tiles, TB, TB), BF16),
            pltpu.VMEM((pairs, tiles, 32, 2 * TB), BF16),
        ],
        compiler_params=pltpu.CompilerParams(vmem_limit_bytes=48 * 1024 * 1024),
    )(x, strength.reshape(1, atoms), tile_pairs)


def shards(positions, strength, tile_pairs, source_segment):
    atom_devices = lax.axis_size("atom")
    img_devices = lax.axis_size("img")
    ring = img_devices * atom_devices
    x = lax.all_to_all(positions, "atom", split_axis=1, concat_axis=2, tiled=True)
    images = x.shape[1]
    images_total = images * ring
    moved = moved_images(x, strength, tile_pairs)
    axes = ("img", "atom")
    before = lax.ppermute(moved[:, -1:], axes, [(i, i + 1) for i in range(ring - 1)])
    after = lax.ppermute(moved[:, :1], axes, [(i + 1, i) for i in range(ring - 1)])
    extended = jnp.concatenate([before, moved, after], axis=1)
    segments = extended[:, 1:-1] - extended[:, :-2]
    squares = jnp.sum(segments * segments, axis=(0, 2))
    everyone = lax.all_gather(squares, axes, axis=0, tiled=True)
    ids = jnp.arange(images_total, dtype=jnp.int32)
    lengths = jnp.where(ids >= 1, jnp.sqrt(1.0 + everyone), 0.0)
    first = (lax.axis_index("img") * atom_devices + lax.axis_index("atom")) * images
    mine = lax.dynamic_slice_in_dim(
        source_segment, lax.axis_index("atom") * images, images, 0
    )
    total_arc = jnp.sum(lengths)
    arc_low = jnp.sum(jnp.where(ids[None, :] < mine[:, None], lengths[None, :], 0.0), axis=1)
    seg_length = jnp.sum(jnp.where(ids[None, :] == mine[:, None], lengths[None, :], 0.0), axis=1)
    own = first + jnp.arange(images, dtype=jnp.int32)
    target = own.astype(F32) * (total_arc / (images_total - 1))
    weight = ((target - arc_low) / seg_length)[None, :, None]
    later = (mine > own)[None, :, None]
    low = jnp.where(later, extended[:, 1:-1], extended[:, :-2])
    high = jnp.where(later, extended[:, 2:], extended[:, 1:-1])
    string = (1.0 - weight) * low + weight * high
    return lax.all_to_all(string, "atom", split_axis=2, concat_axis=1, tiled=True)


def solution(mesh):
    placed = (P(None, "img", "atom"), P(), P(), P("img"))
    return jax.shard_map(
        shards, mesh=mesh, in_specs=placed, out_specs=P(None, "img", "atom"), check_vma=False
    )
```
